256 devices in a mesh: group: 8 (over z), dom: 32 (over y, x, core).
Axes of the slice: x: 4, y: 4, z: 8, core: 2. Of those that a mesh axis runs over, the one named last changes fastest.
Arguments:
- features: bfloat16 [131072, 128], P(('group', 'dom')), may hold values from -6 to 6
- cotangent: bfloat16 [131072, 128], P(('group', 'dom')), may hold values from -6 to 6
- fine_send: int32 [8192, 16], P(('group', 'dom')), may hold values from 0 to 512, as said below
- fine_rim: int32 [512, 128], P(('group', 'dom')), may hold values from 0 to 511
- fine_src: int32 [1048576], P(('group', 'dom')), may hold values from 0 to 1279, as said below
- fine_dst: int32 [1048576], P(('group', 'dom')), may hold values from 0 to 511
- fine_pool: int32 [131072], P(('group', 'dom')), may hold values from 0 to 1023, as said below
- coarse_send: int32 [8192, 4], P(('group', 'dom')), may hold values from 0 to 32, as said below
- coarse_src: int32 [65536], P(('group', 'dom')), may hold values from 0 to 159, as said below
- coarse_dst: int32 [65536], P(('group', 'dom')), may hold values from 0 to 31
- coarse_pool: int32 [8192], P(('group', 'dom')), may hold values from 0 to 511
- w_send: bfloat16 [128, 128], replicated, may hold values from -0.5 to 0.5
- w_recv: bfloat16 [128, 128], replicated, may hold values from -0.5 to 0.5
- w_node: bfloat16 [128, 128], replicated, may hold values from -0.5 to 0.5
- v_send: bfloat16 [128, 128], replicated, may hold values from -0.5 to 0.5
- v_recv: bfloat16 [128, 128], replicated, may hold values from -0.5 to 0.5
- v_node: bfloat16 [128, 128], replicated, may hold values from -0.5 to 0.5
- w_top: bfloat16 [128, 128], replicated, may hold values from -0.5 to 0.5
Outputs:
- flow: bfloat16 [131072, 128], P(('group', 'dom'))
- grad_features: float32 [131072, 128], P(('group', 'dom'))
- grad_send: float32 [128, 128], replicated
The draws below stay inside these ranges and needn't reach their ends.
Inputs may be any that keep to these rules, and one draw needn't show every extreme that they name: `fine_send`: each device holds 32 rows of 16: row p lists own node rows for the device with dom index p of its group; the value 512 marks an empty slot, live slots come first, and three rows of every device are full. `fine_rim`: each device holds two rows: the first go to the previous group's device of the same dom index, the second to the next group's. `fine_src`: index into the device's extended rows: its 512 nodes, 512 rows from its group in dom order, 128 rows from the previous group, 128 from the next. `fine_pool`: coarse node numbered within the node's group. `coarse_send`: as fine_send with 4 slots a row and 32 marking an empty slot. `coarse_src`: index into the device's coarse rows, then 32 * 4 rows from its group in dom order.
All inputs are finite; a program needn't handle non-finite values.
Results may differ from the reference program's by a relative error of at most 0.025.
Values may be sent and summed in bfloat16 or wider, within the bound.
A program may use at most 64 MiB of HBM per device.

```python
import jax
import jax.numpy as jnp
from jax import lax

H = 128
NODE_DEV = 512
EDGE_DEV = 4096
NC_DEV = 32
CEDGE_DEV = 256
SLOT = 16
SLOT_G = 128
CSLOT = 4
NCC = 512
NODES = 131072
N_GROUP = 8
N_DOM = 32


def halo_lists(key, slots, blank_row):
    blocks = N_GROUP * N_DOM * N_DOM
    rows = jax.random.randint(jax.random.fold_in(key, 11), (blocks, slots), 0, blank_row)
    counts = jax.random.randint(jax.random.fold_in(key, 12), (blocks, 1), 1, slots + 1)
    order = jnp.arange(blocks, dtype=jnp.int32)
    device = order // N_DOM
    dom_index = device % N_DOM
    peer = order % N_DOM
    opposite = (dom_index + N_DOM // 2) % N_DOM
    after = (dom_index + 1) % N_DOM
    before = (dom_index + N_DOM - 1) % N_DOM
    full = (peer == opposite) | (peer == after) | (peer == before)
    counts = jnp.where(full[:, None], slots, counts)
    live = jnp.arange(slots, dtype=jnp.int32)[None, :] < counts
    return jnp.where(live, rows, blank_row).astype(jnp.int32)


def edge_sources(key, total, per_device, local_rows, extra_rows, slots):
    near = jax.random.randint(jax.random.fold_in(key, 21), (total,), 0, local_rows)
    far = jax.random.randint(jax.random.fold_in(key, 22), (total,), local_rows, local_rows + extra_rows)
    choose = jax.random.randint(jax.random.fold_in(key, 23), (total,), 0, 8)
    order = jnp.arange(total, dtype=jnp.int32)
    dom_index = order // per_device % N_DOM
    opposite = (dom_index + N_DOM // 2) % N_DOM
    within = jax.random.randint(jax.random.fold_in(key, 24), (total,), 0, slots)
    across = local_rows + opposite * slots + within
    picked = jnp.where(choose < 2, far, jnp.where(choose == 2, across, near))
    return picked.astype(jnp.int32)


def draw_fine_send(key, part):
    return halo_lists(key, SLOT, NODE_DEV)


def draw_coarse_send(key, part):
    return halo_lists(key, CSLOT, NC_DEV)


def draw_fine_src(key, part):
    return edge_sources(key, N_GROUP * N_DOM * EDGE_DEV, EDGE_DEV, NODE_DEV, N_DOM * SLOT + 2 * SLOT_G, SLOT)


def draw_coarse_src(key, part):
    return edge_sources(key, N_GROUP * N_DOM * CEDGE_DEV, CEDGE_DEV, NC_DEV, N_DOM * CSLOT, CSLOT)


def draw_fine_pool(key, part):
    total = N_GROUP * N_DOM * NODE_DEV
    order = jnp.arange(total, dtype=jnp.int32)
    dom_index = order // NODE_DEV % N_DOM
    near = dom_index * NC_DEV + jax.random.randint(jax.random.fold_in(key, 31), (total,), 0, NC_DEV)
    far = jax.random.randint(jax.random.fold_in(key, 32), (total,), 0, NC_DEV * N_DOM)
    choose = jax.random.randint(jax.random.fold_in(key, 33), (total,), 0, 4)
    return jnp.where(choose == 0, far, near).astype(jnp.int32)


def with_ends(array, own_key, least, top_value):
    shape = array.shape
    index_at = [jax.random.randint(jax.random.fold_in(own_key, axis), (), 0, shape[axis]) for axis in range(len(shape))]
    array = array.at[tuple(index_at)].set(least)
    longest = shape.index(max(shape))
    index_at[longest] = (index_at[longest] + 1) % shape[longest]
    return array.at[tuple(index_at)].set(top_value)


def steps_of(stream_key, dims, cuts, low, high):
    factor_of, own = 1.0, jax.random.fold_in(stream_key, 6)
    for position, shards_of in cuts:
        steps = jnp.exp(jax.random.uniform(jax.random.fold_in(own, position), (shards_of,), jnp.float32, low / len(cuts), high / len(cuts)))
        factor_of = factor_of * jnp.repeat(steps, dims[position] // shards_of).reshape([-1 if axis == position else 1 for axis in range(len(dims))])
    return factor_of


def scatter_about(own_key, shape, scale, reach, cuts=(), kind=jnp.bfloat16):
    entries = scale * jax.random.normal(own_key, shape, jnp.float32)
    if cuts:
        entries = entries * steps_of(own_key, shape, cuts, -0.22, 0.18)
    return jnp.clip(entries, -reach, reach).astype(kind)


def setup_inputs(seed: int = 0) -> dict:
    key_list = jax.random.split(jax.random.key(seed), 19)
    features = scatter_about(key_list[0], (NODES, H), 1.0, 6.0, ((0, 256),))
    cotangent = scatter_about(key_list[1], (NODES, H), 1.0, 6.0, ((0, 256),))
    fine_send = draw_fine_send(jax.random.fold_in(key_list[18], 71), 0)
    fine_rim = with_ends(jax.random.randint(key_list[3], (N_GROUP * N_DOM * 2, SLOT_G), 0, NODE_DEV), jax.random.fold_in(key_list[3], 1), 0, NODE_DEV - 1).astype(jnp.int32)
    fine_src = draw_fine_src(jax.random.fold_in(key_list[18], 71), 0)
    fine_dst = with_ends(jax.random.randint(key_list[5], (N_GROUP * N_DOM * EDGE_DEV,), 0, NODE_DEV), jax.random.fold_in(key_list[5], 1), 0, NODE_DEV - 1).astype(jnp.int32)
    fine_pool = draw_fine_pool(jax.random.fold_in(key_list[18], 71), 0)
    coarse_send = draw_coarse_send(jax.random.fold_in(key_list[18], 71), 0)
    coarse_src = draw_coarse_src(jax.random.fold_in(key_list[18], 71), 0)
    coarse_dst = with_ends(jax.random.randint(key_list[9], (N_GROUP * N_DOM * CEDGE_DEV,), 0, NC_DEV), jax.random.fold_in(key_list[9], 1), 0, NC_DEV - 1).astype(jnp.int32)
    coarse_pool = with_ends(jax.random.randint(key_list[10], (N_GROUP * N_DOM * NC_DEV,), 0, NCC), jax.random.fold_in(key_list[10], 1), 0, NCC - 1).astype(jnp.int32)
    w_send = scatter_about(key_list[11], (H, H), H ** -0.5, 0.5)
    w_recv = scatter_about(key_list[12], (H, H), H ** -0.5, 0.5)
    w_node = scatter_about(key_list[13], (H, H), H ** -0.5, 0.5)
    v_send = scatter_about(key_list[14], (H, H), H ** -0.5, 0.5)
    v_recv = scatter_about(key_list[15], (H, H), H ** -0.5, 0.5)
    v_node = scatter_about(key_list[16], (H, H), H ** -0.5, 0.5)
    w_top = scatter_about(key_list[17], (H, H), H ** -0.5, 0.5)
    return dict(features=features, cotangent=cotangent, fine_send=fine_send, fine_rim=fine_rim, fine_src=fine_src, fine_dst=fine_dst, fine_pool=fine_pool, coarse_send=coarse_send, coarse_src=coarse_src, coarse_dst=coarse_dst, coarse_pool=coarse_pool, w_send=w_send, w_recv=w_recv, w_node=w_node, v_send=v_send, v_recv=v_recv, v_node=v_node, w_top=w_top)


def silu_slope(values):
    sigma = jax.nn.sigmoid(values)
    return sigma * (1.0 + values * (1.0 - sigma))


def edge_forward(extended, own_rows, sources, targets, w_send, w_recv, w_node):
    preact = jnp.dot(extended[sources], w_send, preferred_element_type=jnp.float32)
    preact = preact + jnp.dot(own_rows[targets], w_recv, preferred_element_type=jnp.float32)
    message = jax.nn.silu(preact).astype(jnp.bfloat16)
    summed = jax.ops.segment_sum(message.astype(jnp.float32), targets, num_segments=own_rows.shape[0]).astype(jnp.bfloat16)
    updated = (own_rows.astype(jnp.float32) + jnp.dot(summed, w_node, preferred_element_type=jnp.float32)).astype(jnp.bfloat16)
    return updated, preact


def edge_backward(grad_out, extended, own_rows, preact, sources, targets, w_send, w_recv, w_node):
    rounded = grad_out.astype(jnp.bfloat16)
    grad_sum = jnp.dot(rounded, w_node.T, preferred_element_type=jnp.float32)
    grad_pre = (grad_sum[targets] * silu_slope(preact)).astype(jnp.bfloat16)
    grad_ext = jax.ops.segment_sum(jnp.dot(grad_pre, w_send.T, preferred_element_type=jnp.float32), sources, num_segments=extended.shape[0])
    own_count = own_rows.shape[0]
    grad_own = grad_out + jax.ops.segment_sum(jnp.dot(grad_pre, w_recv.T, preferred_element_type=jnp.float32), targets, num_segments=own_count)
    grad_own = grad_own + grad_ext[:own_count]
    grad_weight = lax.dot_general(extended[sources], grad_pre, (((0,), (0,)), ((), ())), preferred_element_type=jnp.float32)
    return grad_own, grad_ext[own_count:], grad_weight


def top_forward(pooled, w_top):
    slope_in = jnp.dot(pooled.astype(jnp.bfloat16), w_top, preferred_element_type=jnp.float32)
    return (pooled + jax.nn.silu(slope_in)).astype(jnp.bfloat16), slope_in


def top_backward(grad_top, slope_in, w_top):
    inner = (grad_top * silu_slope(slope_in)).astype(jnp.bfloat16)
    return grad_top + jnp.dot(inner, w_top.T, preferred_element_type=jnp.float32)


def pick_rows(rows, index):
    return rows[index]


def add_rows(grads, index, values):
    padded = jnp.concatenate([grads, jnp.zeros((1, grads.shape[1]), jnp.float32)], axis=0)
    return padded.at[index].add(values)[:-1]


def reference(features, cotangent, fine_send, fine_rim, fine_src, fine_dst, fine_pool, coarse_send, coarse_src, coarse_dst, coarse_pool, w_send, w_recv, w_node, v_send, v_recv, v_node, w_top):
    group_count = N_GROUP
    dom_count = N_DOM
    devices = group_count * dom_count
    width = features.shape[1]
    pick = jax.vmap(jax.vmap(pick_rows))
    scatter = jax.vmap(jax.vmap(add_rows))
    feats = features.reshape(group_count, dom_count, NODE_DEV, width)
    padded = jnp.concatenate([feats, jnp.zeros((group_count, dom_count, 1, width), jnp.bfloat16)], axis=2)
    send = fine_send.reshape(group_count, dom_count, dom_count, SLOT)
    outgoing = pick(padded, send)
    incoming = jnp.swapaxes(outgoing, 1, 2).reshape(group_count, dom_count, dom_count * SLOT, width)
    layers = pick(feats, fine_rim.reshape(group_count, dom_count, 2, SLOT_G))
    blank = jnp.zeros((1, dom_count, SLOT_G, width), jnp.bfloat16)
    from_prev = jnp.concatenate([blank, layers[:-1, :, 1]], axis=0)
    from_next = jnp.concatenate([layers[1:, :, 0], blank], axis=0)
    extended = jnp.concatenate([feats, incoming, from_prev, from_next], axis=2).reshape(devices, -1, width)
    own = feats.reshape(devices, NODE_DEV, width)
    sources = fine_src.reshape(devices, EDGE_DEV)
    targets = fine_dst.reshape(devices, EDGE_DEV)

    def fine_step(item):
        return edge_forward(item[0], item[1], item[2], item[3], w_send, w_recv, w_node)[0]

    updated = lax.map(fine_step, (extended, own, sources, targets))
    coarse_total = NC_DEV * dom_count
    group_of = jnp.arange(devices * NODE_DEV, dtype=jnp.int32) // (dom_count * NODE_DEV)
    fine_ids = (group_of * coarse_total + fine_pool).astype(jnp.int32)
    pooled_fine = jax.ops.segment_sum(updated.reshape(-1, width).astype(jnp.float32), fine_ids, num_segments=group_count * coarse_total)
    coarse_in = (0.25 * pooled_fine).astype(jnp.bfloat16).reshape(group_count, dom_count, NC_DEV, width)
    cpadded = jnp.concatenate([coarse_in, jnp.zeros((group_count, dom_count, 1, width), jnp.bfloat16)], axis=2)
    csend = coarse_send.reshape(group_count, dom_count, dom_count, CSLOT)
    cincoming = jnp.swapaxes(pick(cpadded, csend), 1, 2).reshape(group_count, dom_count, dom_count * CSLOT, width)
    cextended = jnp.concatenate([coarse_in, cincoming], axis=2).reshape(devices, -1, width)
    cown = coarse_in.reshape(devices, NC_DEV, width)
    csources = coarse_src.reshape(devices, CEDGE_DEV)
    ctargets = coarse_dst.reshape(devices, CEDGE_DEV)

    def coarse_step(item):
        return edge_forward(item[0], item[1], item[2], item[3], v_send, v_recv, v_node)[0]

    coarse_mid = lax.map(coarse_step, (cextended, cown, csources, ctargets)).reshape(-1, width)
    pooled = 0.125 * jax.ops.segment_sum(coarse_mid.astype(jnp.float32), coarse_pool, num_segments=NCC)
    top_out, slope_in = top_forward(pooled, w_top)
    coarse_out = (coarse_mid.astype(jnp.float32) + top_out[coarse_pool].astype(jnp.float32)).astype(jnp.bfloat16)
    flow = (updated.reshape(-1, width).astype(jnp.float32) + coarse_out[fine_ids].astype(jnp.float32)).astype(jnp.bfloat16)

    grad_flow = cotangent.astype(jnp.float32)
    grad_coarse = jax.ops.segment_sum(grad_flow, fine_ids, num_segments=group_count * coarse_total)
    grad_top = jax.ops.segment_sum(grad_coarse, coarse_pool, num_segments=NCC)
    grad_pool = top_backward(grad_top, slope_in, w_top)
    grad_cmid = (grad_coarse + 0.125 * grad_pool[coarse_pool]).reshape(devices, NC_DEV, width)

    def coarse_back(item):
        preact = edge_forward(item[0], item[1], item[2], item[3], v_send, v_recv, v_node)[1]
        result = edge_backward(item[4], item[0], item[1], preact, item[2], item[3], v_send, v_recv, v_node)
        return result[0], result[1]

    c_own, c_halo = lax.map(coarse_back, (cextended, cown, csources, ctargets, grad_cmid))
    creturned = jnp.swapaxes(c_halo.reshape(group_count, dom_count, dom_count, CSLOT, width), 1, 2)
    creturned = creturned.reshape(group_count, dom_count, dom_count * CSLOT, width)
    grad_cin = scatter(c_own.reshape(group_count, dom_count, NC_DEV, width), csend.reshape(group_count, dom_count, dom_count * CSLOT), creturned)
    grad_fmid = (grad_flow + 0.25 * grad_cin.reshape(-1, width)[fine_ids]).reshape(devices, NODE_DEV, width)

    def fine_back(item):
        preact = edge_forward(item[0], item[1], item[2], item[3], w_send, w_recv, w_node)[1]
        return edge_backward(item[4], item[0], item[1], preact, item[2], item[3], w_send, w_recv, w_node)

    f_own, f_halo, f_weight = lax.map(fine_back, (extended, own, sources, targets, grad_fmid))
    grad_send = jnp.sum(f_weight, axis=0)
    split = dom_count * SLOT
    dom_part = f_halo[:, :split].reshape(group_count, dom_count, dom_count, SLOT, width)
    dom_back = jnp.swapaxes(dom_part, 1, 2).reshape(group_count, dom_count, dom_count * SLOT, width)
    grad_x = scatter(f_own.reshape(group_count, dom_count, NODE_DEV, width), send.reshape(group_count, dom_count, dom_count * SLOT), dom_back)
    prev_grad = f_halo[:, split:split + SLOT_G].reshape(group_count, dom_count, SLOT_G, width)
    next_grad = f_halo[:, split + SLOT_G:].reshape(group_count, dom_count, SLOT_G, width)
    blank_grad = jnp.zeros((1, dom_count, SLOT_G, width), jnp.float32)
    to_layer_one = jnp.concatenate([prev_grad[1:], blank_grad], axis=0)
    to_layer_zero = jnp.concatenate([blank_grad, next_grad[:-1]], axis=0)
    rim_values = jnp.stack([to_layer_zero, to_layer_one], axis=2).reshape(group_count, dom_count, 2 * SLOT_G, width)
    grad_x = scatter(grad_x, fine_rim.reshape(group_count, dom_count, 2 * SLOT_G), rim_values)
    return flow, grad_x.reshape(-1, width), grad_send
```

```python
import functools

import jax
import jax.numpy as jnp
from jax import lax
from jax.experimental import pallas as pl
from jax.experimental.pallas import tpu as pltpu
from jax.sharding import PartitionSpec as P

F32 = jnp.float32
BF16 = jnp.bfloat16
MESH = pl.DeviceIdType.MESH

H = 128
NODE = 512
EDGE = 4096
SLOT = 16
RIM = 128
NC = 32
CEDGE = 256
CSLOT = 4
NCC = 512
BLK = 1024

R_SRC, R_DST, R_POOL, R_SEND, R_CSEND, R_CSRC, R_CDST, R_CPOOL = 0, 32, 64, 68, 74, 78, 80, 82
R_ALL = 88


def nn(a, b):
    return jnp.dot(a, b, preferred_element_type=F32)


def nt(a, b):
    return lax.dot_general(a, b, (((1,), (1,)), ((), ())), preferred_element_type=F32)


def tn(a, b):
    return lax.dot_general(a, b, (((0,), (0,)), ((), ())), preferred_element_type=F32)


def hot_rows(count, row, base=0):
    at = lax.broadcasted_iota(jnp.int32, (count, 128), 0) + base
    return jnp.where(at == row, 1.0, 0.0).astype(BF16)


def hot_cols(count, row):
    idx = jnp.transpose(jnp.broadcast_to(row, (128, 128)))
    parts = []
    for m in range(count // 128):
        at = lax.broadcasted_iota(jnp.int32, (128, 128), 1) + 128 * m
        parts.append(jnp.where(at == idx, 1.0, 0.0).astype(BF16))
    return jnp.concatenate(parts, axis=1) if len(parts) > 1 else parts[0]


def gate(v):
    return 0.5 + 0.5 * jnp.tanh(0.5 * v)


def kernel(
    ng, nd,
    feat, cot, idx, w_send, w_recv, w_node, v_send, v_recv, v_node, w_top,
    flow, grad_x, grad_w,
    oht, ohp, ohpr, ohs, ohc, slope, sacc,
    ext, zt, out_a, gsend, gbuf, psend, pbuf, csend, cext, tsend, tbuf, hsend2, hbuf2,
    zsend, zbuf, zsend2, zbuf2, tout, ttab, eout, etab, fsend, fbuf, gout, gtab,
    hsend, hbuf, wsend, wbuf, wmid, wbuf2, wout, wtab,
    ssem, rsem,
):
    g = lax.axis_index("group")
    d = lax.axis_index("dom")

    barrier = pltpu.get_barrier_semaphore()

    def greet_dom(j, c):
        pl.semaphore_signal(barrier, inc=1, device_id=(g, lax.rem(d + j, nd)), device_id_type=MESH)
        return c

    def greet_group(j, c):
        pl.semaphore_signal(barrier, inc=1, device_id=(lax.rem(g + j, ng), d), device_id_type=MESH)
        return c

    lax.fori_loop(1, nd, greet_dom, 0)
    lax.fori_loop(1, ng, greet_group, 0)

    def to_dom(ph, src, dst):
        def step(j, c):
            p = lax.rem(d + j, nd)
            pltpu.make_async_remote_copy(
                src_ref=src(p), dst_ref=dst, send_sem=ssem.at[ph], recv_sem=rsem.at[ph],
                device_id=(g, p), device_id_type=MESH,
            ).start()
            return c

        lax.fori_loop(1, nd, step, 0)

    def to_group(ph, src, dst):
        def step(j, c):
            q = lax.rem(g + j, ng)
            pltpu.make_async_remote_copy(
                src_ref=src(q), dst_ref=dst, send_sem=ssem.at[ph], recv_sem=rsem.at[ph],
                device_id=(q, d), device_id_type=MESH,
            ).start()
            return c

        lax.fori_loop(1, ng, step, 0)

    def to_one(ph, src, dst, q):
        pltpu.make_async_remote_copy(
            src_ref=src, dst_ref=dst, send_sem=ssem.at[ph], recv_sem=rsem.at[ph],
            device_id=(q, d), device_id_type=MESH,
        ).start()

    waits = []

    def arrived(ph, ref):
        pltpu.make_async_copy(ref, ref, rsem.at[ph]).wait()
        waits.append((ph, ref))

    def rows(ref, at, count):
        return ref.at[pl.ds(pl.multiple_of(at, 8), count)]

    ext[0:NODE, :] = feat[...]
    x = feat[...]
    for k in range(6):
        row = idx[R_SEND + k : R_SEND + k + 1, :]
        ohs[:, 128 * k : 128 * k + 128] = hot_rows(NODE, row)
        out_a[128 * k : 128 * k + 128, :] = nn(hot_cols(NODE, row), x).astype(BF16)

    pl.semaphore_wait(barrier, nd - 1 + ng - 1)
    nslot = nd * SLOT
    prev, nxt = lax.rem(g + ng - 1, ng), lax.rem(g + 1, ng)
    to_one(1, out_a.at[nslot : nslot + RIM], ext.at[NODE + nslot + RIM : NODE + nslot + 2 * RIM], prev)
    to_one(1, out_a.at[nslot + RIM : nslot + 2 * RIM], ext.at[NODE + nslot : NODE + nslot + RIM], nxt)
    to_dom(0, lambda p: rows(out_a, p * SLOT, SLOT), rows(ext, NODE + d * SLOT, SLOT))
    rows(ext, NODE + d * SLOT, SLOT)[...] = rows(out_a, d * SLOT, SLOT)[...]

    for k in range(4):
        row = idx[R_POOL + k : R_POOL + k + 1, :]
        ohp[:, 128 * k : 128 * k + 128] = hot_rows(nd * NC, row)
        ohpr[128 * k : 128 * k + 128, :] = hot_cols(nd * NC, row)
    gsend[...] = nn(ohp[...], cot[...]).astype(BF16)
    to_dom(2, lambda p: rows(gsend, p * NC, NC), gbuf.at[d])
    gbuf[d] = rows(gsend, d * NC, NC)[...]

    next_rows = NODE + nslot + 2 * RIM

    def build(b, c):
        for r in range(BLK // 128):
            src = idx[pl.ds(R_SRC + b * (BLK // 128) + r, 1), :]
            dst = idx[pl.ds(R_DST + b * (BLK // 128) + r, 1), :]
            oht[b, 0:next_rows, 128 * r : 128 * r + 128] = hot_rows(next_rows, src)
            oht[b, next_rows : next_rows + NODE, 128 * r : 128 * r + 128] = hot_rows(NODE, dst)
        return c

    lax.fori_loop(0, EDGE // BLK, build, 0)

    c_rows = NC + nd * SLOT
    for k in range(CEDGE // 128):
        src = idx[R_CSRC + k : R_CSRC + k + 1, :]
        dst = idx[R_CDST + k : R_CDST + k + 1, :]
        ohc[0:c_rows, 128 * k : 128 * k + 128] = hot_rows(c_rows, src)
        ohc[c_rows : c_rows + NC, 128 * k : 128 * k + 128] = hot_rows(NC, dst)
    cpool = idx[R_CPOOL : R_CPOOL + 1, :]

    ws_t = jnp.transpose(w_send[...].astype(F32)).astype(BF16)
    wr_t = jnp.transpose(w_recv[...].astype(F32)).astype(BF16)
    vs_t = jnp.transpose(v_send[...].astype(F32)).astype(BF16)
    vr_t = jnp.transpose(v_recv[...].astype(F32)).astype(BF16)
    zt[:, 0:NODE] = nt(ws_t, x).astype(BF16)
    zt[:, next_rows : next_rows + NODE] = nt(wr_t, x).astype(BF16)

    arrived(0, ext.at[0 : (nd - 1) * SLOT])
    arrived(1, ext.at[0 : 2 * RIM])
    at = NODE + nslot
    ext[at : at + RIM, :] = jnp.where(g > 0, ext[at : at + RIM, :].astype(F32), 0.0).astype(BF16)
    ext[at + RIM : at + 2 * RIM, :] = jnp.where(
        g < ng - 1, ext[at + RIM : at + 2 * RIM, :].astype(F32), 0.0
    ).astype(BF16)
    zt[:, NODE:next_rows] = nt(ws_t, ext[NODE:next_rows, :]).astype(BF16)

    def forward(b, total):
        pre = nn(zt[...], oht[b])
        s = gate(pre)
        slope[b] = s * (1.0 + pre * (1.0 - s))
        msg = (pre * s).astype(BF16)
        return total + nt(oht[b, next_rows : next_rows + NODE, :], msg)

    summed = lax.fori_loop(0, EDGE // BLK, forward, jnp.zeros((NODE, H), F32))
    updated = (x.astype(F32) + nn(summed.astype(BF16), w_node[...])).astype(BF16)
    psend[...] = nn(ohp[...], updated).astype(BF16)
    to_dom(3, lambda p: rows(psend, p * NC, NC), pbuf.at[d])
    pbuf[d] = rows(psend, d * NC, NC)[...]

    ohtop = hot_rows(NCC, cpool)[:, 0:NC]
    tb = NCC // nd
    arrived(2, gbuf.at[0 : nd - 1])
    grad_coarse = jnp.sum(gbuf[...].astype(F32), axis=0)
    hsend2[...] = nn(ohtop, grad_coarse.astype(BF16)).astype(BF16)
    to_dom(4, lambda p: rows(hsend2, p * tb, tb), hbuf2.at[d])
    hbuf2[d] = rows(hsend2, d * tb, tb)[...]

    arrived(3, pbuf.at[0 : nd - 1])
    coarse_in = (0.25 * jnp.sum(pbuf[...].astype(F32), axis=0)).astype(BF16)
    ohcs = []
    for k in range(nd * SLOT // 128):
        row = idx[R_CSEND + k : R_CSEND + k + 1, :]
        csend[128 * k : 128 * k + 128, :] = nn(hot_cols(128, row)[:, 0:NC], coarse_in).astype(BF16)
        ohcs.append(hot_rows(NC, row))
    to_dom(5, lambda p: rows(csend, p * SLOT, SLOT), rows(cext, NC + d * SLOT, SLOT))
    cext[0:NC, :] = coarse_in
    rows(cext, NC + d * SLOT, SLOT)[...] = rows(csend, d * SLOT, SLOT)[...]

    arrived(4, hbuf2.at[0 : nd - 1])
    zsend2[...] = jnp.sum(hbuf2[...].astype(F32), axis=0)
    to_group(6, lambda q: zsend2, zbuf2.at[g])
    zbuf2[g] = zsend2[...]

    arrived(5, cext.at[0 : (nd - 1) * SLOT])
    cz = jnp.concatenate(
        [nt(vs_t, cext[...]).astype(BF16), nt(vr_t, coarse_in).astype(BF16)], axis=1
    )
    cpre = nn(cz, ohc[...])
    cs = gate(cpre)
    cslope = cs * (1.0 + cpre * (1.0 - cs))
    csum = nt(ohc[c_rows : c_rows + NC, :], (cpre * cs).astype(BF16))
    coarse_mid = (coarse_in.astype(F32) + nn(csum.astype(BF16), v_node[...])).astype(BF16)
    tsend[...] = nn(ohtop, coarse_mid).astype(BF16)
    to_dom(7, lambda p: rows(tsend, p * tb, tb), tbuf.at[d])
    tbuf[d] = rows(tsend, d * tb, tb)[...]

    arrived(6, zbuf2.at[0 : ng - 1])
    grad_top = jnp.sum(zbuf2[...], axis=0)

    arrived(7, tbuf.at[0 : nd - 1])
    zsend[...] = jnp.sum(tbuf[...].astype(F32), axis=0)
    to_group(8, lambda q: zsend, zbuf.at[g])
    zbuf[g] = zsend[...]
    arrived(8, zbuf.at[0 : ng - 1])
    pooled = 0.125 * jnp.sum(zbuf[...], axis=0)
    slope_in = nn(pooled.astype(BF16), w_top[...])
    ts = gate(slope_in)
    tout[0:tb, :] = (pooled + slope_in * ts).astype(BF16)
    inner = (grad_top * (ts * (1.0 + slope_in * (1.0 - ts)))).astype(BF16)
    tout[tb : 2 * tb, :] = (grad_top + nt(inner, w_top[...])).astype(BF16)
    to_dom(9, lambda p: tout, rows(ttab, d * 2 * tb, 2 * tb))
    rows(ttab, d * 2 * tb, 2 * tb)[...] = tout[...]

    lane = lax.broadcasted_iota(jnp.int32, (1, 128), 1)
    spot = (cpool // tb) * (2 * tb) + lax.rem(cpool, tb) + jnp.where(lane >= NC, tb, 0)
    picker = hot_cols(2 * NCC, jnp.where(lane < 2 * NC, spot, -1))
    arrived(9, ttab.at[0 : (nd - 1) * 2 * tb])
    picked = nn(picker, ttab[...])
    coarse_out = coarse_mid.astype(F32) + picked[0:NC, :]
    eout[...] = coarse_out.astype(BF16)
    to_dom(10, lambda p: eout, rows(etab, d * NC, NC))
    rows(etab, d * NC, NC)[...] = eout[...]

    grad_cmid = grad_coarse + 0.125 * picked[NC : 2 * NC, :]
    cgs = nt(v_node[...], grad_cmid.astype(BF16)).astype(BF16)
    cgp = (nn(cgs, ohc[c_rows : c_rows + NC, :]) * cslope).astype(BF16)
    csc = nt(ohc[...], cgp).astype(BF16)
    cge = nt(csc[0:c_rows, :], v_send[...])
    fsend[...] = cge[NC:c_rows, :].astype(BF16)
    to_dom(11, lambda p: rows(fsend, p * SLOT, SLOT), rows(fbuf, d * SLOT, SLOT))
    rows(fbuf, d * SLOT, SLOT)[...] = rows(fsend, d * SLOT, SLOT)[...]
    c_own = grad_cmid + nt(csc[c_rows : c_rows + NC, :], v_recv[...]) + cge[0:NC, :]
    ohcs = jnp.concatenate(ohcs, axis=1)
    arrived(11, fbuf.at[0 : (nd - 1) * SLOT])
    gout[...] = (c_own + nn(ohcs, fbuf[...])).astype(BF16)
    to_dom(12, lambda p: gout, rows(gtab, d * NC, NC))
    rows(gtab, d * NC, NC)[...] = gout[...]

    arrived(10, etab.at[0 : (nd - 1) * NC])
    flow[...] = (updated.astype(F32) + nn(ohpr[...], etab[...])).astype(BF16)

    arrived(12, gtab.at[0 : (nd - 1) * NC])
    grad_mid = cot[...].astype(F32) + 0.25 * nn(ohpr[...], gtab[...])
    gs = nt(w_node[...], grad_mid.astype(BF16)).astype(BF16)
    sacc[...] = jnp.zeros_like(sacc)

    def backward(b, c):
        gp = (nn(gs, oht[b, next_rows : next_rows + NODE, :]) * slope[b]).astype(BF16)
        sacc[...] += nt(oht[b], gp)
        return c

    lax.fori_loop(0, EDGE // BLK, backward, 0)
    s_src = sacc[0:next_rows, :].astype(BF16)
    wb = H // ng
    wsend[...] = tn(ext[...], s_src)
    to_group(13, lambda q: rows(wsend, q * wb, wb), wbuf.at[g])
    wbuf[g] = rows(wsend, g * wb, wb)[...]

    gext = nt(s_src, w_send[...])
    hsend[...] = gext[NODE:, :].astype(BF16)
    to_one(15, hsend.at[nslot : nslot + RIM], hbuf.at[nslot + RIM : nslot + 2 * RIM], prev)
    to_one(15, hsend.at[nslot + RIM : nslot + 2 * RIM], hbuf.at[nslot : nslot + RIM], nxt)
    to_dom(14, lambda p: rows(hsend, p * SLOT, SLOT), rows(hbuf, d * SLOT, SLOT))
    rows(hbuf, d * SLOT, SLOT)[...] = rows(hsend, d * SLOT, SLOT)[...]
    s_dst = sacc[next_rows : next_rows + NODE, :].astype(BF16)
    grad_x[...] = grad_mid + nt(s_dst, w_recv[...]) + gext[0:NODE, :]

    arrived(13, wbuf.at[0 : ng - 1])
    wmid[...] = jnp.sum(wbuf[...], axis=0)
    to_dom(16, lambda p: wmid, wbuf2.at[d])
    wbuf2[d] = wmid[...]

    arrived(14, hbuf.at[0 : (nd - 1) * SLOT])
    arrived(15, hbuf.at[0 : 2 * RIM])
    hbuf[nslot : nslot + RIM, :] = jnp.where(
        g > 0, hbuf[nslot : nslot + RIM, :].astype(F32), 0.0
    ).astype(BF16)
    hbuf[nslot + RIM : nslot + 2 * RIM, :] = jnp.where(
        g < ng - 1, hbuf[nslot + RIM : nslot + 2 * RIM, :].astype(F32), 0.0
    ).astype(BF16)
    grad_x[...] += nn(ohs[...], hbuf[...])

    arrived(16, wbuf2.at[0 : nd - 1])
    wout[...] = jnp.sum(wbuf2[...], axis=0)
    to_group(17, lambda q: wout, rows(wtab, g * wb, wb))
    rows(wtab, g * wb, wb)[...] = wout[...]
    arrived(17, wtab.at[0 : (ng - 1) * wb])
    grad_w[...] = wtab[...]

    for ph, ref in waits:
        pltpu.make_async_copy(ref, ref, ssem.at[ph]).wait()


def solution(mesh):
    ng, nd = mesh.shape["group"], mesh.shape["dom"]
    nslot = nd * SLOT
    ext_rows = NODE + nslot + 2 * RIM
    c_rows = NC + nslot
    tb, wb = NCC // nd, H // ng

    def local(
        features, cotangent, fine_send, fine_rim, fine_src, fine_dst, fine_pool,
        coarse_send, coarse_src, coarse_dst, coarse_pool,
        w_send, w_recv, w_node, v_send, v_recv, v_node, w_top,
    ):
        far = coarse_src - NC
        csrc = jnp.where(far < 0, coarse_src, NC + (far // CSLOT) * SLOT + far % CSLOT)
        csend = jnp.pad(coarse_send, ((0, 0), (0, SLOT - CSLOT)), constant_values=NC)
        cpool = jnp.tile(coarse_pool, 128 // NC)
        idx = jnp.concatenate(
            [
                fine_src, fine_dst, fine_pool, fine_send.reshape(-1), fine_rim.reshape(-1),
                csend.reshape(-1), csrc, coarse_dst, cpool,
                jnp.zeros((R_ALL - R_CPOOL - 1) * 128, jnp.int32),
            ]
        ).reshape(R_ALL, 128)
        vm = pl.BlockSpec(memory_space=pltpu.VMEM)
        return pl.pallas_call(
            functools.partial(kernel, ng, nd),
            out_shape=(
                jax.ShapeDtypeStruct((NODE, H), BF16),
                jax.ShapeDtypeStruct((NODE, H), F32),
                jax.ShapeDtypeStruct((H, H), F32),
            ),
            in_specs=[vm] * 10,
            out_specs=(vm, vm, vm),
            scratch_shapes=[
                pltpu.VMEM((EDGE // BLK, ext_rows + NODE, BLK), BF16),
                pltpu.VMEM((nd * NC, NODE), BF16),
                pltpu.VMEM((NODE, nd * NC), BF16),
                pltpu.VMEM((NODE, nslot + 2 * RIM), BF16),
                pltpu.VMEM((c_rows + NC, CEDGE), BF16),
                pltpu.VMEM((EDGE // BLK, H, BLK), F32),
                pltpu.VMEM((ext_rows + NODE, H), F32),
                pltpu.VMEM((ext_rows, H), BF16),
                pltpu.VMEM((H, ext_rows + NODE), BF16),
                pltpu.VMEM((nslot + 2 * RIM, H), BF16),
                pltpu.VMEM((nd * NC, H), BF16),
                pltpu.VMEM((nd, NC, H), BF16),
                pltpu.VMEM((nd * NC, H), BF16),
                pltpu.VMEM((nd, NC, H), BF16),
                pltpu.VMEM((nslot, H), BF16),
                pltpu.VMEM((c_rows, H), BF16),
                pltpu.VMEM((NCC, H), BF16),
                pltpu.VMEM((nd, tb, H), BF16),
                pltpu.VMEM((NCC, H), BF16),
                pltpu.VMEM((nd, tb, H), BF16),
                pltpu.VMEM((tb, H), F32),
                pltpu.VMEM((ng, tb, H), F32),
                pltpu.VMEM((tb, H), F32),
                pltpu.VMEM((ng, tb, H), F32),
                pltpu.VMEM((2 * tb, H), BF16),
                pltpu.VMEM((2 * NCC, H), BF16),
                pltpu.VMEM((NC, H), BF16),
                pltpu.VMEM((nd * NC, H), BF16),
                pltpu.VMEM((nslot, H), BF16),
                pltpu.VMEM((nslot, H), BF16),
                pltpu.VMEM((NC, H), BF16),
                pltpu.VMEM((nd * NC, H), BF16),
                pltpu.VMEM((nslot + 2 * RIM, H), BF16),
                pltpu.VMEM((nslot + 2 * RIM, H), BF16),
                pltpu.VMEM((H, H), F32),
                pltpu.VMEM((ng, wb, H), F32),
                pltpu.VMEM((wb, H), F32),
                pltpu.VMEM((nd, wb, H), F32),
                pltpu.VMEM((wb, H), F32),
                pltpu.VMEM((H, H), F32),
                pltpu.SemaphoreType.DMA((18,)),
                pltpu.SemaphoreType.DMA((18,)),
            ],
            compiler_params=pltpu.CompilerParams(
                collective_id=0, has_side_effects=True, vmem_limit_bytes=60 * 1024 * 1024
            ),
        )(features, cotangent, idx, w_send, w_recv, w_node, v_send, v_recv, v_node, w_top)

    both = P(("group", "dom"))
    rows = P(("group", "dom"), None)
    in_specs = (rows, rows, rows, rows, both, both, both, rows, both, both, both) + (P(),) * 7
    return jax.shard_map(
        local, mesh=mesh, in_specs=in_specs, out_specs=(rows, rows, P()), check_vma=False
    )
```

```python
import functools

import jax
import jax.numpy as jnp
from jax import lax
from jax.experimental import pallas as pl
from jax.experimental.pallas import tpu as pltpu
from jax.sharding import PartitionSpec as P

F32 = jnp.float32
BF16 = jnp.bfloat16
I32 = jnp.int32
MESH = pl.DeviceIdType.MESH

H = 128
NODE = 512
EDGE = 4096
SLOT = 16
RIM = 128
NC = 32
CEDGE = 256
CSLOT = 4
BLK = 1024
NB = EDGE // BLK

(A, RZ, IX, IZ, GB, PB, GA, CH, ZG, MA, ZT, CR, GC, CO, W1, HR, HZ, W2, W3) = range(19)


def nn(a, b):
    return jnp.dot(a, b, preferred_element_type=F32)


def nt(a, b):
    return lax.dot_general(a, b, (((1,), (1,)), ((), ())), preferred_element_type=F32)


def one_where(mask):
    return jnp.where(mask, 1.0, 0.0).astype(BF16)


def hot_rows(count, row):
    return one_where(lax.broadcasted_iota(I32, (count, 128), 0) == row)


def down(row):
    return jnp.transpose(jnp.broadcast_to(row, (128, 128)))


def hot_cols(count, row):
    idx = down(row)
    at = lax.broadcasted_iota(I32, (128, 128), 1)
    parts = [one_where(at + 128 * m == idx) for m in range(count // 128)]
    return jnp.concatenate(parts, axis=1) if len(parts) > 1 else parts[0]


def gate(v):
    return 0.5 + 0.5 * jnp.tanh(0.5 * v)


def turned(w):
    return jnp.transpose(w.astype(F32)).astype(BF16)


def kernel(
    ng, nd, *refs,
):
    n_in = 18
    hbm = refs[:n_in]
    flow, grad_x, grad_w = refs[n_in : n_in + 3]
    vin = refs[n_in + 3 : 2 * n_in + 3]
    (
        oht, ohp, ohpr, ohs, ohc, ohcs, quest, slope, gpre, srcs, sacc, ext, zt, wide,
        out_a, cp_out, cp_all, cp_z, gsend, gbuf, psend, pbuf, gcout, gctab, csend, cext,
        zgsend, zgbuf, mout, mtab, zsend, zbuf, fsend, fbuf, gout, gtab, eout, etab,
        wsend, wbuf, wmid, wbuf2, wout, wtab, hsend, hbuf, isem, ssem, rsem,
    ) = refs[2 * n_in + 3 :]
    (
        feat, cot, f_send, f_rim, f_src, f_dst, f_pool, c_send, c_src, c_dst, c_pool,
        w_send, w_recv, w_node, v_send, v_recv, v_node, w_top,
    ) = vin

    g = lax.axis_index("group")
    d = lax.axis_index("dom")

    barrier = pltpu.get_barrier_semaphore()

    def greet_dom(j, c):
        pl.semaphore_signal(barrier, inc=1, device_id=(g, lax.rem(d + j, nd)), device_id_type=MESH)
        return c

    def greet_group(j, c):
        pl.semaphore_signal(barrier, inc=1, device_id=(lax.rem(g + j, ng), d), device_id_type=MESH)
        return c

    order = (0, 2, 3, 10, 4, 5, 6, 1, 11, 12, 7, 8, 9, 13, 14, 15, 16, 17)
    for i in order:
        pltpu.make_async_copy(hbm[i], vin[i], isem.at[i]).start()
    lax.fori_loop(1, nd, greet_dom, 0)
    lax.fori_loop(1, ng, greet_group, 0)

    def fetched(*which):
        for i in which:
            pltpu.make_async_copy(hbm[i], vin[i], isem.at[i]).wait()

    def push(ph, src, dst, device):
        pltpu.make_async_remote_copy(
            src_ref=src, dst_ref=dst, send_sem=ssem.at[ph], recv_sem=rsem.at[ph],
            device_id=device, device_id_type=MESH,
        ).start()

    def to_dom(ph, src, dst):
        def step(j, c):
            p = lax.rem(d + j, nd)
            push(ph, src(p), dst, (g, p))
            return c

        lax.fori_loop(nd // 2, nd, step, 0)
        lax.fori_loop(1, nd // 2, step, 0)

    def to_group(ph, src, dst):
        def step(j, c):
            q = lax.rem(g + j, ng)
            push(ph, src(q), dst, (q, d))
            return c

        lax.fori_loop(ng // 2, ng, step, 0)
        lax.fori_loop(1, ng // 2, step, 0)

    waits = []

    def arrived(ph, ref):
        pltpu.make_async_copy(ref, ref, rsem.at[ph]).wait()
        waits.append((ph, ref))

    def rows(ref, at, count):
        return ref.at[pl.ds(pl.multiple_of(at, 8), count)]

    lane = lax.broadcasted_iota(I32, (1, 128), 1)
    nslot = nd * SLOT
    halo = nslot + 2 * RIM
    own = 2 * NODE
    total = own + halo
    c_rows = NC + nslot
    prev, nxt = lax.rem(g + ng - 1, ng), lax.rem(g + 1, ng)

    def flat(ref, count, fill):
        wide[0:SLOT, :] = jnp.full((SLOT, 128), fill, I32)
        wide[0:count, 0:nd] = ref[...]
        t = jnp.transpose(wide[...])[0:nd, :]
        for s in (SLOT, 2 * SLOT, 4 * SLOT):
            t = t + pltpu.roll(t, s, 1)
        at = lax.broadcasted_iota(I32, (nd, 128), 0) & 7
        t = jnp.where(lax.broadcasted_iota(I32, (nd, 128), 1) // SLOT == at, t, 0)
        return [
            jnp.sum(t[8 * k : 8 * k + 8, :], axis=0, keepdims=True) for k in range(nslot // 128)
        ]

    wide[...] = jnp.zeros_like(wide)
    fetched(0, 2, 3, 10)
    x = feat[...]
    send_rows = flat(f_send, SLOT, 0) + [f_rim[0:1, :], f_rim[1:2, :]]
    for k, row in enumerate(send_rows):
        out_a[128 * k : 128 * k + 128, :] = nn(hot_cols(NODE, row), x).astype(BF16)
    cp = jnp.concatenate([c_pool[...]] * (128 // NC), axis=1)
    cp_out[...] = cp

    pl.semaphore_wait(barrier, nd - 1 + ng - 1)
    to_dom(A, lambda p: rows(out_a, p * SLOT, SLOT), rows(ext, NODE + d * SLOT, SLOT))
    push(RZ, out_a.at[nslot : nslot + RIM], ext.at[NODE + nslot + RIM : NODE + halo], (prev, d))
    push(RZ, out_a.at[nslot + RIM : halo], ext.at[NODE + nslot : NODE + nslot + RIM], (nxt, d))
    to_group(IZ, lambda q: cp_out, cp_z.at[g])
    to_dom(IX, lambda p: cp_out, cp_all.at[d])
    rows(ext, NODE + d * SLOT, SLOT)[...] = rows(out_a, d * SLOT, SLOT)[...]
    cp_all[d] = cp
    cp_z[g] = cp
    ext[0:NODE, :] = x

    fetched(4, 5)

    def build(b, c):
        for r in range(BLK // 128):
            src = f_src[pl.ds(b * (BLK // 128) + r, 1), :]
            dst = f_dst[pl.ds(b * (BLK // 128) + r, 1), :]
            oht[b, 0:NODE, 128 * r : 128 * r + 128] = hot_rows(NODE, dst)
            oht[b, NODE:total, 128 * r : 128 * r + 128] = hot_rows(total - NODE, src)
        return c

    lax.fori_loop(0, NB, build, 0)

    fetched(11, 12)
    ws_t, wr_t = turned(w_send[...]), turned(w_recv[...])
    zt[:, 0:NODE] = nt(wr_t, x).astype(BF16)
    zt[:, NODE:own] = nt(ws_t, x).astype(BF16)

    def begin(b, c):
        slope[b] = nn(zt[:, 0:own], oht[b, 0:own, :])
        return c

    lax.fori_loop(0, NB, begin, 0)

    fetched(6, 1)
    for k in range(NODE // 128):
        row = f_pool[k : k + 1, :]
        ohp[:, 128 * k : 128 * k + 128] = hot_rows(nd * NC, row)
    gsend[...] = nn(ohp[...], cot[...]).astype(BF16)
    fetched(7, 8, 9, 13, 14, 15, 16, 17)

    arrived(A, ext.at[0 : (nd - 1) * SLOT])
    arrived(RZ, ext.at[0 : 2 * RIM])
    at = NODE + nslot
    ext[at : at + RIM, :] = jnp.where(g > 0, ext[at : at + RIM, :].astype(F32), 0.0).astype(BF16)
    ext[at + RIM : at + 2 * RIM, :] = jnp.where(
        g < ng - 1, ext[at + RIM : at + 2 * RIM, :].astype(F32), 0.0
    ).astype(BF16)
    zt[:, own:total] = nt(ws_t, ext[NODE : NODE + halo, :]).astype(BF16)
    to_dom(GB, lambda p: rows(gsend, p * NC, NC), gbuf.at[d])
    gbuf[d] = rows(gsend, d * NC, NC)[...]
    sacc[0:NODE, :] = jnp.zeros((NODE, H), F32)

    def forward(b, c):
        pre = slope[b] + nn(zt[:, own:total], oht[b, own:total, :])
        s = gate(pre)
        slope[b] = s * (1.0 + pre * (1.0 - s))
        msg = (pre * s).astype(BF16)
        sacc[0:NODE, :] += nt(oht[b, 0:NODE, :], msg)
        return c

    lax.fori_loop(0, NB, forward, 0)
    updated = (x.astype(F32) + nn(sacc[0:NODE, :].astype(BF16), w_node[...])).astype(BF16)
    psend[...] = nn(ohp[...], updated).astype(BF16)
    to_dom(PB, lambda p: rows(psend, p * NC, NC), pbuf.at[d])
    pbuf[d] = rows(psend, d * NC, NC)[...]

    arrived(GB, gbuf.at[0 : nd - 1])
    grad_coarse = jnp.sum(gbuf[...].astype(F32), axis=0)
    gcout[...] = grad_coarse.astype(BF16)
    to_dom(GA, lambda p: gcout, rows(gctab, d * NC, NC))
    rows(gctab, d * NC, NC)[...] = gcout[...]

    send_c = flat(c_send, CSLOT, NC)
    for k, row in enumerate(send_c):
        ohcs[:, 128 * k : 128 * k + 128] = hot_rows(NC, row)
    for k in range(CEDGE // 128):
        src = c_src[k : k + 1, :]
        far = src - NC
        src = jnp.where(far < 0, src, NC + (far >> 2) * SLOT + (far & 3))
        ohc[0:c_rows, 128 * k : 128 * k + 128] = hot_rows(c_rows, src)
        ohc[c_rows : c_rows + NC, 128 * k : 128 * k + 128] = hot_rows(NC, c_dst[k : k + 1, :])
    outs_c = [hot_cols(128, row)[:, 0:NC] for row in send_c]
    vs_t, vr_t = turned(v_send[...]), turned(v_recv[...])

    arrived(PB, pbuf.at[0 : nd - 1])
    coarse_in = (0.25 * jnp.sum(pbuf[...].astype(F32), axis=0)).astype(BF16)
    for k in range(nslot // 128):
        csend[128 * k : 128 * k + 128, :] = nn(outs_c[k], coarse_in).astype(BF16)
    to_dom(CH, lambda p: rows(csend, p * SLOT, SLOT), rows(cext, NC + d * SLOT, SLOT))
    cext[0:NC, :] = coarse_in
    rows(cext, NC + d * SLOT, SLOT)[...] = rows(csend, d * SLOT, SLOT)[...]

    arrived(IX, cp_all.at[0 : nd - 1])
    arrived(IZ, cp_z.at[0 : ng - 1])

    def joined(ref, k):
        row = ref[4 * k]
        for a in range(1, 4):
            row = jnp.where(lane // NC == a, ref[4 * k + a], row)
        return row

    for k in range(ng * NC // 128):
        want = down(joined(cp_z, k))
        for m in range(nd * NC // 128):
            quest[128 * k : 128 * k + 128, 128 * m : 128 * m + 128] = one_where(
                want == joined(cp_all, m)
            )

    arrived(GA, gctab.at[0 : (nd - 1) * NC])
    zgsend[...] = nn(quest[...], gctab[...]).astype(BF16)
    to_group(ZG, lambda q: rows(zgsend, q * NC, NC), zgbuf.at[g])
    zgbuf[g] = rows(zgsend, g * NC, NC)[...]

    arrived(CH, cext.at[0 : (nd - 1) * SLOT])
    cz = jnp.concatenate(
        [nt(vs_t, cext[...]).astype(BF16), nt(vr_t, coarse_in).astype(BF16)], axis=1
    )
    cpre = nn(cz, ohc[...])
    cs = gate(cpre)
    cslope = cs * (1.0 + cpre * (1.0 - cs))
    csum = nt(ohc[c_rows : c_rows + NC, :], (cpre * cs).astype(BF16))
    coarse_mid = coarse_in.astype(F32) + nn(csum.astype(BF16), v_node[...])
    mout[...] = coarse_mid.astype(BF16)
    to_dom(MA, lambda p: mout, rows(mtab, d * NC, NC))
    rows(mtab, d * NC, NC)[...] = mout[...]
    coarse_mid = mout[...].astype(F32)

    ext_t = jnp.transpose(ext[...].astype(F32)).astype(BF16)

    def pick(b, c):
        srcs[b] = nn(ext_t, oht[b, NODE:total, :]).astype(BF16)
        return c

    lax.fori_loop(0, NB, pick, 0)
    arrived(ZG, zgbuf.at[0 : ng - 1])
    grad_top = jnp.sum(zgbuf[...].astype(F32), axis=0)

    arrived(MA, mtab.at[0 : (nd - 1) * NC])
    zsend[...] = nn(quest[...], mtab[...]).astype(BF16)
    to_group(ZT, lambda q: rows(zsend, q * NC, NC), zbuf.at[g])
    zbuf[g] = rows(zsend, g * NC, NC)[...]
    for k in range(NODE // 128):
        ohpr[128 * k : 128 * k + 128, :] = hot_cols(nd * NC, f_pool[k : k + 1, :])
    arrived(ZT, zbuf.at[0 : ng - 1])
    pooled = 0.125 * jnp.sum(zbuf[...].astype(F32), axis=0)
    slope_in = nn(pooled.astype(BF16), w_top[...])
    ts = gate(slope_in)
    top_out = (pooled + slope_in * ts).astype(BF16)
    inner = (grad_top * (ts * (1.0 + slope_in * (1.0 - ts)))).astype(BF16)
    grad_pool = grad_top + nt(inner, w_top[...])

    grad_cmid = grad_coarse + 0.125 * grad_pool
    cgs = nt(v_node[...], grad_cmid.astype(BF16)).astype(BF16)
    cgp = (nn(cgs, ohc[c_rows : c_rows + NC, :]) * cslope).astype(BF16)
    csc = nt(ohc[...], cgp).astype(BF16)
    cge = nt(csc[0:c_rows, :], v_send[...])
    fsend[...] = cge[NC:c_rows, :].astype(BF16)
    to_dom(CR, lambda p: rows(fsend, p * SLOT, SLOT), rows(fbuf, d * SLOT, SLOT))
    rows(fbuf, d * SLOT, SLOT)[...] = rows(fsend, d * SLOT, SLOT)[...]
    c_own = grad_cmid + nt(csc[c_rows : c_rows + NC, :], v_recv[...]) + cge[0:NC, :]
    for k, row in enumerate(send_rows):
        ohs[:, 128 * k : 128 * k + 128] = hot_rows(NODE, row)
    eout[...] = (coarse_mid + top_out.astype(F32)).astype(BF16)
    arrived(CR, fbuf.at[0 : (nd - 1) * SLOT])
    gout[...] = (c_own + nn(ohcs[...], fbuf[...])).astype(BF16)
    to_dom(GC, lambda p: gout, rows(gtab, d * NC, NC))
    rows(gtab, d * NC, NC)[...] = gout[...]

    arrived(GC, gtab.at[0 : (nd - 1) * NC])
    to_dom(CO, lambda p: eout, rows(etab, d * NC, NC))
    rows(etab, d * NC, NC)[...] = eout[...]
    grad_mid = cot[...].astype(F32) + 0.25 * nn(ohpr[...], gtab[...])
    gs = nt(w_node[...], grad_mid.astype(BF16)).astype(BF16)

    def edges(b, acc):
        gp = (nn(gs, oht[b, 0:NODE, :]) * slope[b]).astype(BF16)
        gpre[b] = gp
        return acc + nt(srcs[b], gp)

    wb = H // ng
    wsend[...] = lax.fori_loop(0, NB, edges, jnp.zeros((H, H), F32)).astype(BF16)
    to_group(W1, lambda q: rows(wsend, q * wb, wb), wbuf.at[g])
    wbuf[g] = rows(wsend, g * wb, wb)[...]

    sacc[...] = jnp.zeros_like(sacc)

    def back_halo(b, c):
        sacc[own:total, :] += nt(oht[b, own:total, :], gpre[b])
        return c

    lax.fori_loop(0, NB, back_halo, 0)
    hsend[...] = nt(sacc[own:total, :].astype(BF16), w_send[...]).astype(BF16)
    to_dom(HR, lambda p: rows(hsend, p * SLOT, SLOT), rows(hbuf, d * SLOT, SLOT))
    push(HZ, hsend.at[nslot : nslot + RIM], hbuf.at[nslot + RIM : halo], (prev, d))
    push(HZ, hsend.at[nslot + RIM : halo], hbuf.at[nslot : nslot + RIM], (nxt, d))
    rows(hbuf, d * SLOT, SLOT)[...] = rows(hsend, d * SLOT, SLOT)[...]

    arrived(W1, wbuf.at[0 : ng - 1])
    wmid[...] = jnp.sum(wbuf[...].astype(F32), axis=0).astype(BF16)
    to_dom(W2, lambda p: wmid, wbuf2.at[d])
    wbuf2[d] = wmid[...]

    def back_own(b, c):
        sacc[0:own, :] += nt(oht[b, 0:own, :], gpre[b])
        return c

    lax.fori_loop(0, NB, back_own, 0)
    s_own = sacc[0:own, :].astype(BF16)
    grad_x[...] = grad_mid + nt(s_own[0:NODE, :], w_recv[...]) + nt(s_own[NODE:own, :], w_send[...])
    arrived(CO, etab.at[0 : (nd - 1) * NC])
    flow[...] = (updated.astype(F32) + nn(ohpr[...], etab[...])).astype(BF16)

    arrived(W2, wbuf2.at[0 : nd - 1])
    wout[...] = jnp.sum(wbuf2[...].astype(F32), axis=0)
    to_group(W3, lambda q: wout, rows(wtab, g * wb, wb))
    rows(wtab, g * wb, wb)[...] = wout[...]

    arrived(HR, hbuf.at[0 : (nd - 1) * SLOT])
    arrived(HZ, hbuf.at[0 : 2 * RIM])
    hbuf[nslot : nslot + RIM, :] = jnp.where(
        g > 0, hbuf[nslot : nslot + RIM, :].astype(F32), 0.0
    ).astype(BF16)
    hbuf[nslot + RIM : halo, :] = jnp.where(
        g < ng - 1, hbuf[nslot + RIM : halo, :].astype(F32), 0.0
    ).astype(BF16)
    grad_x[...] += nn(ohs[...], hbuf[...])

    for ph, ref in waits:
        pltpu.make_async_copy(ref, ref, ssem.at[ph]).wait()
    arrived(W3, wtab.at[0 : (ng - 1) * wb])
    grad_w[...] = wtab[...]
    pltpu.make_async_copy(waits[-1][1], waits[-1][1], ssem.at[W3]).wait()


def write_out(*refs):
    sem = refs[-1]
    copies = [pltpu.make_async_copy(refs[i], refs[3 + i], sem.at[i]) for i in range(3)]
    for c in copies:
        c.start()
    for c in copies:
        c.wait()


def solution(mesh):
    ng, nd = mesh.shape["group"], mesh.shape["dom"]
    nslot = nd * SLOT
    halo = nslot + 2 * RIM
    total = 2 * NODE + halo
    c_rows = NC + nslot
    wb = H // ng
    pooled = nd * NC

    def local(
        features, cotangent, fine_send, fine_rim, fine_src, fine_dst, fine_pool,
        coarse_send, coarse_src, coarse_dst, coarse_pool,
        w_send, w_recv, w_node, v_send, v_recv, v_node, w_top,
    ):
        args = (
            features, cotangent, fine_send.T, fine_rim,
            fine_src.reshape(-1, 128), fine_dst.reshape(-1, 128), fine_pool.reshape(-1, 128),
            coarse_send.T, coarse_src.reshape(-1, 128), coarse_dst.reshape(-1, 128),
            coarse_pool.reshape(1, -1),
            w_send, w_recv, w_node, v_send, v_recv, v_node, w_top,
        )
        scratch = [pltpu.VMEM(a.shape, a.dtype) for a in args] + [
            pltpu.VMEM((NB, total, BLK), BF16),
            pltpu.VMEM((pooled, NODE), BF16),
            pltpu.VMEM((NODE, pooled), BF16),
            pltpu.VMEM((NODE, halo), BF16),
            pltpu.VMEM((c_rows + NC, CEDGE), BF16),
            pltpu.VMEM((NC, nslot), BF16),
            pltpu.VMEM((ng * NC, pooled), BF16),
            pltpu.VMEM((NB, H, BLK), F32),
            pltpu.VMEM((NB, H, BLK), BF16),
            pltpu.VMEM((NB, H, BLK), BF16),
            pltpu.VMEM((total, H), F32),
            pltpu.VMEM((NODE + halo, H), BF16),
            pltpu.VMEM((H, total), BF16),
            pltpu.VMEM((128, 128), I32),
            pltpu.VMEM((halo, H), BF16),
            pltpu.VMEM((1, 128), I32),
            pltpu.VMEM((nd, 1, 128), I32),
            pltpu.VMEM((ng, 1, 128), I32),
            pltpu.VMEM((pooled, H), BF16),
            pltpu.VMEM((nd, NC, H), BF16),
            pltpu.VMEM((pooled, H), BF16),
            pltpu.VMEM((nd, NC, H), BF16),
            pltpu.VMEM((NC, H), BF16),
            pltpu.VMEM((pooled, H), BF16),
            pltpu.VMEM((nslot, H), BF16),
            pltpu.VMEM((c_rows, H), BF16),
            pltpu.VMEM((ng * NC, H), BF16),
            pltpu.VMEM((ng, NC, H), BF16),
            pltpu.VMEM((NC, H), BF16),
            pltpu.VMEM((pooled, H), BF16),
            pltpu.VMEM((ng * NC, H), BF16),
            pltpu.VMEM((ng, NC, H), BF16),
            pltpu.VMEM((nslot, H), BF16),
            pltpu.VMEM((nslot, H), BF16),
            pltpu.VMEM((NC, H), BF16),
            pltpu.VMEM((pooled, H), BF16),
            pltpu.VMEM((NC, H), BF16),
            pltpu.VMEM((pooled, H), BF16),
            pltpu.VMEM((H, H), BF16),
            pltpu.VMEM((ng, wb, H), BF16),
            pltpu.VMEM((wb, H), BF16),
            pltpu.VMEM((nd, wb, H), BF16),
            pltpu.VMEM((wb, H), F32),
            pltpu.VMEM((H, H), F32),
            pltpu.VMEM((halo, H), BF16),
            pltpu.VMEM((halo, H), BF16),
            pltpu.SemaphoreType.DMA((len(args),)),
            pltpu.SemaphoreType.DMA((19,)),
            pltpu.SemaphoreType.DMA((19,)),
        ]
        vm = pl.BlockSpec(memory_space=pltpu.VMEM)
        anywhere = pl.BlockSpec(memory_space=pl.ANY)
        shapes = (((NODE, H), BF16), ((NODE, H), F32), ((H, H), F32))
        parts = pl.pallas_call(
            functools.partial(kernel, ng, nd),
            out_shape=tuple(pltpu.VMEM(s, t) for s, t in shapes),
            in_specs=[anywhere] * len(args),
            out_specs=(vm, vm, vm),
            scratch_shapes=scratch,
            compiler_params=pltpu.CompilerParams(
                collective_id=0, has_side_effects=True, vmem_limit_bytes=58 * 1024 * 1024
            ),
        )(*args)
        return pl.pallas_call(
            write_out,
            out_shape=tuple(jax.ShapeDtypeStruct(s, t) for s, t in shapes),
            in_specs=[vm, vm, vm],
            out_specs=(anywhere, anywhere, anywhere),
            scratch_shapes=[pltpu.SemaphoreType.DMA((3,))],
        )(*[pltpu.with_memory_space_constraint(p, pltpu.VMEM) for p in parts])

    both = P(("group", "dom"))
    rows = P(("group", "dom"), None)
    in_specs = (rows, rows, rows, rows, both, both, both, rows, both, both, both) + (P(),) * 7
    return jax.shard_map(
        local, mesh=mesh, in_specs=in_specs, out_specs=(rows, rows, P()), check_vma=False
    )
```
